256 devices in a mesh: dp: 32 (over y, z_hi, x), expert: 8 (over z_lo, core).
Axes of the slice: x: 4, y: 4, z: 8 (z_hi: 2, z_lo: 4; z = z_hi * 4 + z_lo), core: 2. Of those that a mesh axis runs over, the one named last changes fastest.
Arguments:
- tokens: bfloat16 [32768, 1024], P(('dp', 'expert')), may hold values from -24 to 24
- route_first: int32 [32768, 1], P(('dp', 'expert')), may hold values from 0 to 1; in each aligned block of 128 rows (0 to 127, 128 to 255, ...) at most 68 rows name the same one
- route_second: int32 [32768, 1], P(('dp', 'expert')), may hold values from 0 to 3; in each aligned block of 128 rows (0 to 127, 128 to 255, ...) at most 34 rows name the same one
- up_first: bfloat16 [8, 1024, 1024], P('expert', 'dp'), may hold values from -0.1875 to 0.1875
- down_first: bfloat16 [8, 1024, 1024], P('expert', 'dp'), may hold values from -0.09375 to 0.09375
- up_second: bfloat16 [8, 1024, 2048], P('expert', 'dp'), may hold values from -0.1875 to 0.1875
- down_second: bfloat16 [8, 2048, 1024], P('expert', 'dp'), may hold values from -0.09375 to 0.09375
- cotangent: bfloat16 [32768, 1024], P(('dp', 'expert')), may hold values from -6 to 6
Outputs:
- layer_out: bfloat16 [32768, 1024], P(('dp', 'expert'))
- grad_tokens: bfloat16 [32768, 1024], P(('dp', 'expert'))
- grad_up_first: float32 [8, 1024, 1024], P('expert', 'dp')
- grad_down_first: float32 [8, 1024, 1024], P('expert', 'dp')
- grad_up_second: float32 [8, 1024, 2048], P('expert', 'dp')
- grad_down_second: float32 [8, 2048, 1024], P('expert', 'dp')
The draws below stay inside these ranges and needn't reach their ends.
Inputs may be any that keep to these rules, and one draw needn't show every extreme that they name: `route_first`: in each aligned block of 128 rows (the rows of one device) no expert id appears more than 68 times, and in every draw some expert appears exactly 68 times in some block. `route_second`: in each aligned block of 128 rows (the rows of one device) no expert id appears more than 34 times, and in every draw some expert appears exactly 34 times in some block.
All inputs are finite; a program needn't handle non-finite values.
Results may differ from the reference program's by a relative error of at most 0.025.
Values may be sent and summed in bfloat16 or wider, within the bound.
No kernel may reach another device: no remote copies, remote signals or barrier semaphores. Data moves between devices by JAX's collectives and lax.ppermute only.
A program may use at most 128 MiB of HBM per device.

```python
import math
import jax
import jax.numpy as jnp
import numpy as np
from jax import lax

D = 1024
FF = 4096
TOK_DEV = 128
TOKENS = 32768
EXP_A = 2
HID_A = 1024
CAP_A = 68
EXP_B = 4
HID_B = 2048
CAP_B = 34
N_DP = 32
N_EXPERT = 8


def draw_tokens(key, part):
    keys = jax.random.split(jax.random.fold_in(key, 11), 3)
    row_scale = jnp.exp(jax.random.uniform(keys[0], (TOKENS, 1), jnp.float32, jnp.log(0.3), jnp.log(3.0)))
    column_scale = jnp.exp(jax.random.uniform(keys[1], (1, D), jnp.float32, jnp.log(0.5), jnp.log(2.0)))
    values = jnp.clip(jax.random.normal(keys[2], (TOKENS, D), jnp.float32), -4.0, 4.0)
    return (values * row_scale * column_scale).astype(jnp.bfloat16)


def shard_levels(key, dims, cuts, smallest, largest):
    def one(axis_at, blocks):
        heights = jax.random.uniform(jax.random.fold_in(jax.random.fold_in(key, 6), axis_at), (blocks,), jnp.float32, smallest / len(cuts), largest / len(cuts))
        return jnp.repeat(jnp.exp(heights), dims[axis_at] // blocks).reshape((-1,) + (1,) * (len(dims) - axis_at - 1))

    loudness = one(*cuts[0])
    for cut in cuts[1:]:
        loudness = loudness * one(*cut)
    return loudness


def assign_block(own_key, own, number, rows, count, top, bound, lean):
    sequence = jax.random.permutation(own_key, count)
    heavy_load, usual = portions_of(count, rows * top, bound, lean, True), portions_of(count, rows * top, bound, lean, False)
    places = jnp.arange(count)

    def named(tallies, offset_by):
        used = int((tallies > 0).sum())
        fixed = max(1, used // 4)
        shifted = fixed + (places - fixed + offset_by * (used - fixed)) % max(1, count - fixed)
        return jnp.zeros((count,), jnp.int32).at[sequence[jnp.where(places < fixed, places, shifted)]].set(jnp.asarray(tallies, jnp.int32))

    tallies = jnp.where(number % 4 == 0, named(heavy_load, number // 4), named(usual, number - number // 4 - 1))
    mixed = jax.random.permutation(jax.random.fold_in(own, 3), count)
    giver, receiver = mixed[0:count // 2 * 2:2], mixed[1:count // 2 * 2:2]
    room = jnp.minimum(tallies[giver] - 1, bound - tallies[receiver]) // 2
    room = jnp.where((giver == sequence[0]) | (receiver == sequence[0]) | (tallies[receiver] == 0), 0, jnp.maximum(room, 0))
    shifted = jax.random.randint(jax.random.fold_in(own, 4), (count // 2,), 0, 1 << 20) % (room + 1)
    tallies = tallies.at[giver].add(-shifted).at[receiver].add(shifted)
    members = jnp.searchsorted(jnp.cumsum(tallies), jnp.arange(rows * top), side="right").astype(jnp.int32)
    listing = members.reshape(top, rows).T
    listing = listing[jax.random.permutation(jax.random.fold_in(own, 1), rows)]
    offset_by = jax.random.randint(jax.random.fold_in(own, 2), (rows, 1), 0, top)
    return jnp.take_along_axis(listing, (jnp.arange(top)[None, :] + offset_by) % top, axis=1)


def portions_of(number_of, total, bound, skew, full):
    loads = [(1 << 20) // math.isqrt(standing ** skew) + 1 for standing in range(1, number_of + 1)]
    largest = bound if full else min(bound, max(-(-total // number_of), total * loads[0] // sum(loads)))
    least = 1 if total - largest >= number_of - 1 else 0
    holding, rest = [largest] + [least] * (number_of - 1), total - largest - least * (number_of - 1)
    while rest > 0:
        movable = [i for i in range(1, number_of) if holding[i] < largest] or [i for i in range(1, number_of) if holding[i] < bound]
        pool, left = sum([loads[i] for i in movable]), rest
        for i in movable:
            addition = min(bound - holding[i], max(1, left * loads[i] // pool), rest)
            holding[i] = holding[i] + addition
            rest = rest - addition
    return np.array(holding)


def centred(rng, extent, scale, bound, cuts=(), kind=jnp.bfloat16):
    drawn = scale * jax.random.normal(rng, extent, jnp.float32)
    if cuts:
        drawn = drawn * shard_levels(rng, extent, cuts, -0.22, 0.18)
    return jnp.clip(drawn, -bound, bound).astype(kind)


def setup_inputs(seed: int = 0) -> dict:
    splits = jax.random.split(jax.random.key(seed), 9)
    tokens = draw_tokens(jax.random.fold_in(splits[8], 71), 0)
    route_first_keys = jax.random.split(jax.random.fold_in(splits[1], 1), TOKENS // TOK_DEV)
    route_first_turns = jax.random.permutation(jax.random.fold_in(splits[1], 3), TOKENS // TOK_DEV)
    route_first = jax.vmap(lambda own, number: assign_block(jax.random.fold_in(splits[1], 2), own, number, TOK_DEV, EXP_A, 1, CAP_A, 2))(route_first_keys, route_first_turns).reshape((TOKENS, 1))
    route_second_keys = jax.random.split(jax.random.fold_in(splits[2], 1), TOKENS // TOK_DEV)
    route_second_turns = jax.random.permutation(jax.random.fold_in(splits[2], 3), TOKENS // TOK_DEV)
    route_second = jax.vmap(lambda own, number: assign_block(jax.random.fold_in(splits[2], 2), own, number, TOK_DEV, EXP_B, 1, CAP_B, 2))(route_second_keys, route_second_turns).reshape((TOKENS, 1))
    up_first = centred(splits[3], (N_EXPERT, D, HID_A), D ** -0.5, 0.1875, ((0, 8), (1, 32)))
    down_first = centred(splits[4], (N_EXPERT, HID_A, D), FF ** -0.5, 0.09375, ((0, 8), (1, 32)))
    up_second = centred(splits[5], (N_EXPERT, D, HID_B), D ** -0.5, 0.1875, ((0, 8), (1, 32)))
    down_second = centred(splits[6], (N_EXPERT, HID_B, D), FF ** -0.5, 0.09375, ((0, 8), (1, 32)))
    cotangent = centred(splits[7], (TOKENS, D), 1.0, 6.0, ((0, 256),))
    return dict(tokens=tokens, route_first=route_first, route_second=route_second, up_first=up_first, down_first=down_first, up_second=up_second, down_second=down_second, cotangent=cotangent)


epsilon = 1e-06

def rms_normal(widened):
    return widened * lax.rsqrt(lax.optimization_barrier(jnp.mean(widened * widened, axis=-1, keepdims=True)) + epsilon)

def gelu_slope(pre_gelu):
    _, pullback = jax.vjp(jax.nn.gelu, pre_gelu)
    return pullback(jnp.ones_like(pre_gelu))[0]

def slot_places(route_ids, experts, capacity):
    expert_ids = route_ids[:, 0].reshape(-1, TOK_DEV)
    onehot = (expert_ids[:, :, None] == jnp.arange(experts, dtype=jnp.int32)[None, None, :]).astype(jnp.int32)
    earlier = jnp.cumsum(onehot, axis=1) - onehot
    return expert_ids * capacity + lax.optimization_barrier(jnp.sum(earlier * onehot, axis=2))

def spread(token_rows, places, experts, capacity):
    feature_count = token_rows.shape[1]
    blocks = token_rows.reshape(-1, TOK_DEV, feature_count)

    def place_block(block, block_places):
        return jnp.zeros((experts * capacity, feature_count), block.dtype).at[block_places].set(block)
    filled = jax.vmap(place_block)(blocks, places)
    return filled.reshape(N_DP, N_EXPERT, experts, capacity, feature_count)

def pick_rows(slot_table, block_places):
    return slot_table[block_places]

def collect(parts, places, experts):
    group_size = N_EXPERT // experts
    capacity = parts.shape[3]
    feature_count = parts.shape[4]
    summed = parts.astype(jnp.float32).reshape(experts, group_size, N_DP, N_EXPERT, capacity, feature_count).sum(axis=1)
    summed = jnp.transpose(summed, (1, 2, 0, 3, 4)).reshape(N_DP * N_EXPERT, experts * capacity, feature_count)
    picked = jax.vmap(pick_rows)(summed, places)
    return picked.reshape(-1, feature_count)

def column_inputs(buffers, column, group_size):
    return lax.dynamic_index_in_dim(buffers, column // group_size, axis=2, keepdims=False).astype(jnp.float32)

def layer_forward(token_rows, route_ids, up_full, down_full, experts, capacity):
    group_size = N_EXPERT // experts
    places = slot_places(route_ids, experts, capacity)
    widened = token_rows.astype(jnp.float32)
    normed = rms_normal(widened).astype(jnp.bfloat16)
    buffers = spread(normed, places, experts, capacity)

    def forward_column(column_args):
        column, up_one, down_one = column_args
        received = column_inputs(buffers, column, group_size)
        pre_gelu = jnp.einsum('abkd,dh->abkh', received, up_one.astype(jnp.float32))
        hidden = lax.optimization_barrier(jax.nn.gelu(pre_gelu).astype(jnp.bfloat16)).astype(jnp.float32)
        return jnp.einsum('abkh,hd->abkd', hidden, down_one.astype(jnp.float32)).astype(jnp.bfloat16)
    columns = jnp.arange(N_EXPERT, dtype=jnp.int32)
    parts = lax.map(forward_column, (columns, up_full, down_full))
    branch = collect(parts, places, experts)
    return ((widened + branch).astype(jnp.bfloat16), (widened, places, buffers))

def layer_backward(upstream, saved, up_full, down_full, experts, capacity):
    widened, places, buffers = saved
    group_size = N_EXPERT // experts
    arrivals = spread(upstream, places, experts, capacity)

    def backward_column(column_args):
        column, up_one, down_one = column_args
        received = column_inputs(buffers, column, group_size)
        arriving = column_inputs(arrivals, column, group_size)
        up_wide = up_one.astype(jnp.float32)
        down_wide = down_one.astype(jnp.float32)
        pre_gelu = jnp.einsum('abkd,dh->abkh', received, up_wide)
        hidden = lax.optimization_barrier(jax.nn.gelu(pre_gelu).astype(jnp.bfloat16)).astype(jnp.float32)
        grad_pre = (jnp.einsum('abkd,hd->abkh', arriving, down_wide) * gelu_slope(pre_gelu)).astype(jnp.bfloat16)
        grad_wide = lax.optimization_barrier(grad_pre).astype(jnp.float32)
        down_rows = jnp.einsum('abkh,abkd->ahd', hidden, arriving)
        grad_down = lax.optimization_barrier(down_rows.astype(jnp.bfloat16)).astype(jnp.float32).sum(axis=0)
        up_rows = jnp.einsum('abkd,abkh->adh', received, grad_wide)
        grad_up = lax.optimization_barrier(up_rows.astype(jnp.bfloat16)).astype(jnp.float32).sum(axis=0)
        grad_slots = jnp.einsum('abkh,dh->abkd', grad_wide, up_wide).astype(jnp.bfloat16)
        return (grad_up, grad_down, grad_slots)
    columns = jnp.arange(N_EXPERT, dtype=jnp.int32)
    grad_ups, grad_downs, slot_grads = lax.map(backward_column, (columns, up_full, down_full))
    grad_normed = collect(slot_grads, places, experts)
    _, pullback = jax.vjp(rms_normal, widened)
    grad_input = (upstream.astype(jnp.float32) + pullback(grad_normed)[0]).astype(jnp.bfloat16)
    return (grad_input, grad_ups, grad_downs)

def reference(tokens, route_first, route_second, up_first, down_first, up_second, down_second, cotangent):
    middle, first_saved = layer_forward(tokens, route_first, up_first, down_first, EXP_A, CAP_A)
    layer_out, second_saved = layer_forward(middle, route_second, up_second, down_second, EXP_B, CAP_B)
    grad_middle, grad_up_second, grad_down_second = layer_backward(cotangent, second_saved, up_second, down_second, EXP_B, CAP_B)
    grad_tokens, grad_up_first, grad_down_first = layer_backward(grad_middle, first_saved, up_first, down_first, EXP_A, CAP_A)
    return (layer_out, grad_tokens, grad_up_first, grad_down_first, grad_up_second, grad_down_second)
```

```python
import functools

import jax
import jax.numpy as jnp
from jax import lax
from jax.experimental import pallas as pl
from jax.experimental.pallas import tpu as pltpu
from jax.sharding import Mesh, PartitionSpec as P

epsilon = 1e-06
AXES = ("y", "zh", "x", "zl", "core")
SIZES = {"y": 4, "zh": 2, "x": 4, "zl": 4, "core": 2}
bf16, f32 = jnp.bfloat16, jnp.float32


def shift(value, axis, by):
    n = SIZES[axis]
    return lax.ppermute(value, axis, [(i, (i + by) % n) for i in range(n)])


def swap(value, axis, mask):
    return lax.ppermute(value, axis, [(i, i ^ mask) for i in range(SIZES[axis])])


def add(*values):
    total = values[0].astype(f32)
    for v in values[1:]:
        total = total + v.astype(f32)
    return total


def gather_pieces(block, inner, outer):
    near = jnp.concatenate([block] + [shift(block, inner, d) for d in (1, 2, 3)], axis=0)
    below = shift(near, outer, 1)
    above = shift(near, outer, 3)
    half = near.shape[0] // 2
    far_low = shift(below[:half], outer, 1)
    far_high = shift(above[half:], outer, 3)
    return near, below, above, far_low, far_high


def sources(rows, inner_is_x, position):
    y, zh, x = position
    inner, outer = (x, y) if inner_is_x else (y, x)
    for piece, by in ((0, 0), (1, 3), (2, 1), (3, 2)):
        o = (outer + by) % 4
        for j in range(4):
            i = (inner + 4 - j) % 4
            yy, xx = (o, i) if inner_is_x else (i, o)
            for k in range(2):
                at = j * 2 + k
                which = piece
                if piece == 3 and at >= 4:
                    which, at = 4, at - 4
                block = yy * 8 + ((zh + k) % 2) * 4 + xx
                yield which, at * rows, block * rows


def assemble_kernel(rows, inner_is_x, position_ref, *refs):
    pieces, out_ref, sems = refs[:5], refs[5], refs[6]
    position = (position_ref[0], position_ref[1], position_ref[2])
    copies = []
    for n, (which, start, to) in enumerate(sources(rows, inner_is_x, position)):
        copy = pltpu.make_async_copy(
            pieces[which].at[pl.ds(start, rows)],
            out_ref.at[pl.ds(pl.multiple_of(to, rows), rows)],
            sems.at[n],
        )
        copy.start()
        copies.append(copy)
    for copy in copies:
        copy.wait()


def assemble(pieces, rows, inner_is_x, position):
    columns = pieces[0].shape[1]
    return pl.pallas_call(
        functools.partial(assemble_kernel, rows, inner_is_x),
        out_shape=jax.ShapeDtypeStruct((32 * rows, columns), bf16),
        in_specs=[pl.BlockSpec(memory_space=pltpu.SMEM)]
        + [pl.BlockSpec(memory_space=pltpu.HBM)] * 5,
        out_specs=pl.BlockSpec(memory_space=pltpu.VMEM),
        scratch_shapes=[pltpu.SemaphoreType.DMA((32,))],
    )(position, *pieces)


def take(blocks, index, axis):
    return lax.dynamic_index_in_dim(blocks, index, axis, keepdims=False)


def reduce_ring(blocks, axis, position):
    here, ahead, far, behind = (take(blocks, (position + d) % 4, 0) for d in range(4))
    from_below = shift(far[:1], axis, 1)
    from_above = shift(far[1:], axis, 3)
    ahead = jnp.concatenate([add(ahead[:1], from_below).astype(bf16), ahead[1:]], axis=0)
    behind = jnp.concatenate([behind[:1], add(behind[1:], from_above).astype(bf16)], axis=0)
    return add(here, shift(ahead, axis, 1), shift(behind, axis, 3)).astype(bf16)


def reduce_direct(blocks, axis, position):
    own = [take(blocks, (position + d) % 4, 0) for d in range(4)]
    return add(own[0], *[shift(own[d], axis, d) for d in (1, 2, 3)]).astype(bf16)


def reduce_pair(first, second, position):
    y, zh, x = position
    r, c = first.shape[0] // 32, first.shape[1]
    a = jnp.transpose(first.reshape(4, 2, 4, r, c), (0, 1, 2, 3, 4))
    a = reduce_ring(a, "y", y)
    a = reduce_direct(jnp.transpose(a, (1, 0, 2, 3)), "x", x)
    r2, c2 = second.shape[0] // 32, second.shape[1]
    b = jnp.transpose(second.reshape(4, 2, 4, r2, c2), (2, 1, 0, 3, 4))
    b = reduce_ring(b, "x", x)
    b = reduce_direct(jnp.transpose(b, (1, 0, 2, 3)), "y", y)
    out = []
    for v in (a, b):
        out.append(add(take(v, zh, 0), swap(take(v, 1 - zh, 0), "zh", 1)))
    return out


def slot_order(route_ids, experts):
    expert_ids = route_ids[:, 0]
    n = expert_ids.shape[0]
    onehot = (expert_ids[:, None] == jnp.arange(experts, dtype=jnp.int32)[None, :]).astype(bf16)
    row = lax.broadcasted_iota(jnp.int32, (n, n), 0)
    column = lax.broadcasted_iota(jnp.int32, (n, n), 1)
    earlier = jnp.dot((column < row).astype(bf16), onehot, preferred_element_type=f32)
    count = jnp.sum(earlier * onehot.astype(f32), axis=1)
    return expert_ids, count.astype(jnp.int32)


def to_slots(rows, places, slots):
    table = (places[None, :] == jnp.arange(slots, dtype=jnp.int32)[:, None]).astype(rows.dtype)
    return jnp.dot(table, rows, preferred_element_type=f32).astype(rows.dtype)


def from_slots(slot_rows, places):
    slots = slot_rows.shape[0]
    table = (places[:, None] == jnp.arange(slots, dtype=jnp.int32)[None, :]).astype(bf16)
    return jnp.dot(table, slot_rows, preferred_element_type=f32)


def spread_first(slots):
    n = slots.shape[0] // 2
    mine = jnp.concatenate([slots[:n], swap(slots[n:], "zl", 2)], axis=0)
    mine = jnp.concatenate([mine, swap(mine, "zl", 1)], axis=0)
    return jnp.concatenate([mine, swap(mine, "core", 1)], axis=0)


def collect_first(parts):
    for axis, mask in (("core", 1), ("zl", 1)):
        n = parts.shape[0] // 2
        parts = add(parts[:n], swap(parts[n:], axis, mask)).astype(bf16)
    n = parts.shape[0] // 2
    return jnp.concatenate([parts[:n], swap(parts[n:], "zl", 2)], axis=0)


def exchange_second(slots):
    n = slots.shape[0] // 4
    return jnp.concatenate(
        [slots[:n]] + [swap(slots[k * n : (k + 1) * n], "zl", k) for k in (1, 2, 3)], axis=0
    )


def spread_second(slots):
    mine = exchange_second(slots)
    return jnp.concatenate([mine, swap(mine, "core", 1)], axis=0)


def collect_second(parts):
    n = parts.shape[0] // 2
    return exchange_second(add(parts[:n], swap(parts[n:], "core", 1)).astype(bf16))


def rms_normal(widened):
    return widened * lax.rsqrt(jnp.mean(widened * widened, axis=-1, keepdims=True) + epsilon)


def gelu_slope(pre_gelu):
    _, pullback = jax.vjp(jax.nn.gelu, pre_gelu)
    return pullback(jnp.ones_like(pre_gelu))[0]


def mm(a, b, contract):
    return lax.dot_general(a, b, (contract, ((), ())), preferred_element_type=f32)


def local(tokens, route_first, route_second, up_1, down_1, up_2, down_2, cotangent):
    y, zh, x = (lax.axis_index(a) for a in ("y", "zh", "x"))
    zl = lax.axis_index("zl")
    position = jnp.stack([y, zh, x]).astype(jnp.int32)
    up_1, down_1, up_2, down_2 = up_1[0], down_1[0], up_2[0], down_2[0]

    def both_zh(block):
        return jnp.concatenate([block, swap(block, "zh", 1)], axis=0)

    r1 = up_1.shape[0]
    other = swap(jnp.concatenate([up_1, down_1], axis=0), "zh", 1)
    up_1_pieces = gather_pieces(jnp.concatenate([up_1, other[:r1]], axis=0), "x", "y")
    down_1_pieces = gather_pieces(jnp.concatenate([down_1, other[r1:]], axis=0), "y", "x")
    up_1_full = assemble(up_1_pieces, r1, True, position)
    down_1_full = assemble(down_1_pieces, r1, False, position)

    r2, r3 = up_2.shape[0], down_2.shape[0]
    up_2_full = assemble(gather_pieces(both_zh(up_2), "x", "y"), r2, True, position)
    down_2_full = assemble(gather_pieces(both_zh(down_2), "y", "x"), r3, False, position)

    n_1, n_2 = 72, 40
    expert_1, count_1 = slot_order(route_first, 2)
    expert_2, count_2 = slot_order(route_second, 4)
    places_1 = (expert_1 ^ (zl // 2)) * n_1 + count_1
    places_2 = (expert_2 ^ zl) * n_2 + count_2

    wide_1 = tokens.astype(f32)
    received_1 = spread_first(to_slots(rms_normal(wide_1).astype(bf16), places_1, 2 * n_1))
    arriving_2 = spread_second(to_slots(cotangent, places_2, 4 * n_2))
    pre_1 = mm(received_1, up_1_full, ((1,), (0,)))
    hidden_1 = jax.nn.gelu(pre_1).astype(bf16)
    part_1 = mm(hidden_1, down_1_full, ((1,), (0,))).astype(bf16)
    middle = (wide_1 + from_slots(collect_first(part_1), places_1)).astype(bf16)

    wide_2 = middle.astype(f32)
    received_2 = spread_second(to_slots(rms_normal(wide_2).astype(bf16), places_2, 4 * n_2))
    pre_2 = mm(received_2, up_2_full, ((1,), (0,)))
    hidden_2 = jax.nn.gelu(pre_2).astype(bf16)
    part_2 = mm(hidden_2, down_2_full, ((1,), (0,))).astype(bf16)
    layer_out = (wide_2 + from_slots(collect_second(part_2), places_2)).astype(bf16)

    grad_pre_2 = (mm(arriving_2, down_2_full, ((1,), (1,))) * gelu_slope(pre_2)).astype(bf16)
    grad_slots_2 = mm(grad_pre_2, up_2_full, ((1,), (1,))).astype(bf16)
    grad_down_2 = mm(hidden_2, arriving_2, ((0,), (0,))).astype(bf16)
    grad_up_2 = mm(received_2, grad_pre_2, ((0,), (0,))).astype(bf16)
    grad_normed_2 = from_slots(collect_second(grad_slots_2), places_2)
    _, pullback_2 = jax.vjp(rms_normal, wide_2)
    grad_middle = (cotangent.astype(f32) + pullback_2(grad_normed_2)[0]).astype(bf16)

    arriving_1 = spread_first(to_slots(grad_middle, places_1, 2 * n_1))
    grad_pre_1 = (mm(arriving_1, down_1_full, ((1,), (1,))) * gelu_slope(pre_1)).astype(bf16)
    grad_slots_1 = mm(grad_pre_1, up_1_full, ((1,), (1,))).astype(bf16)
    grad_down_1 = mm(hidden_1, arriving_1, ((0,), (0,))).astype(bf16)
    grad_up_1 = mm(received_1, grad_pre_1, ((0,), (0,))).astype(bf16)
    grad_normed_1 = from_slots(collect_first(grad_slots_1), places_1)
    _, pullback_1 = jax.vjp(rms_normal, wide_1)
    grad_tokens = (grad_middle.astype(f32) + pullback_1(grad_normed_1)[0]).astype(bf16)

    out_up_2, out_down_2 = reduce_pair(grad_up_2, grad_down_2, (y, zh, x))
    out_up_1, out_down_1 = reduce_pair(grad_up_1, grad_down_1, (y, zh, x))
    return (layer_out, grad_tokens, out_up_1[None], out_down_1[None], out_up_2[None], out_down_2[None])


def solution(mesh):
    fine = Mesh(mesh.devices.reshape(tuple(SIZES.values())), AXES)
    rows = P(AXES, None)
    weights = P(("zl", "core"), ("y", "zh", "x"), None)
    in_specs = (rows, rows, rows, weights, weights, weights, weights, rows)
    out_specs = (rows, rows, weights, weights, weights, weights)
    return jax.shard_map(local, mesh=fine, in_specs=in_specs, out_specs=out_specs, check_vma=False)
```

```python
import functools

import jax
import jax.numpy as jnp
from jax import lax
from jax.experimental import pallas as pl
from jax.experimental.pallas import tpu as pltpu
from jax.sharding import Mesh, PartitionSpec as P


epsilon = 1e-06
AXES = ("y", "zh", "x", "zl", "core")
SIZES = {"y": 4, "zh": 2, "x": 4, "zl": 4, "core": 2}
bf16, f32 = jnp.bfloat16, jnp.float32


def shift(value, axis, by):
    n = SIZES[axis]
    return lax.ppermute(value, axis, [(i, (i + by) % n) for i in range(n)])


def swap(value, axis, mask):
    return lax.ppermute(value, axis, [(i, i ^ mask) for i in range(SIZES[axis])])


def add(*values):
    total = values[0].astype(f32)
    for v in values[1:]:
        total = total + v.astype(f32)
    return total


def stack_kernel(groups, *refs):
    ins, outs = refs[: sum(groups)], refs[sum(groups) :]
    n = 0
    for count, out in zip(groups, outs):
        rows = out.shape[0] // count
        for k in range(count):
            out[k * rows : (k + 1) * rows, :] = ins[n][...]
            n += 1


def stack(*groups):
    blocks = [block for group in groups for block in group]
    out_shape = [
        jax.ShapeDtypeStruct((len(g) * g[0].shape[0], g[0].shape[1]), g[0].dtype) for g in groups
    ]
    return pl.pallas_call(
        functools.partial(stack_kernel, [len(g) for g in groups]),
        out_shape=out_shape,
        in_specs=[pl.BlockSpec(memory_space=pltpu.VMEM)] * len(blocks),
        out_specs=[pl.BlockSpec(memory_space=pltpu.VMEM)] * len(groups),
    )(*blocks)


def sources(rows, inner_is_x, position):
    y, zh, x = position
    inner, outer = (x, y) if inner_is_x else (y, x)
    for piece, by in ((0, 0), (1, 3), (2, 1), (3, 2)):
        o = (outer + by) % 4
        for j in range(4):
            i = (inner + 4 - j) % 4
            yy, xx = (o, i) if inner_is_x else (i, o)
            for k in range(2):
                block = yy * 8 + ((zh + k) % 2) * 4 + xx
                yield piece, (j * 2 + k) * rows, block * rows


def assemble_kernel(rows, position_ref, *refs):
    position = (position_ref[0], position_ref[1], position_ref[2])
    for pieces, out_ref, inner_is_x in ((refs[:4], refs[8], True), (refs[4:8], refs[9], False)):
        for which, start, to in sources(rows, inner_is_x, position):
            at = pl.ds(pl.multiple_of(to, rows), rows)
            out_ref[at, :] = pieces[which][start : start + rows, :]


def assemble(first, second, rows, position):
    shape = jax.ShapeDtypeStruct((32 * rows, first[0].shape[1]), bf16)
    return pl.pallas_call(
        functools.partial(assemble_kernel, rows),
        out_shape=[shape, shape],
        in_specs=[pl.BlockSpec(memory_space=pltpu.SMEM)]
        + [pl.BlockSpec(memory_space=pltpu.VMEM)] * 8,
        out_specs=[pl.BlockSpec(memory_space=pltpu.VMEM)] * 2,
    )(position, *first, *second)


def gather_first(up, down, position):
    rows = up.shape[0]
    block = jnp.concatenate([up, down], axis=0)
    other = swap(block, "zh", 1)
    a, b = stack((up, other[:rows]), (down, other[rows:]))
    a = [a] + [shift(a, "x", d) for d in (1, 2, 3)]
    b = [b] + [shift(b, "y", d) for d in (1, 2, 3)]
    a, b = stack(a, b)
    a = [a, shift(a, "y", 1), shift(a, "y", 3)]
    b = [b, shift(b, "x", 1), shift(b, "x", 3)]
    a.append(shift(a[1], "y", 1))
    b.append(shift(b[1], "x", 1))
    return assemble(a, b, rows, position)


def parts_of_line(zh, r, width):
    for device in range(16):
        yy, xx = device // 4, device % 4
        for k in range(2):
            block = yy * 8 + ((zh + k) % 2) * 4 + xx
            line = (device * 2 + k) * 4 * r
            yield line, 0, block * r, 0, r
            yield line + r, 0, block * r, width, r
            yield line + 2 * r, 1, block * 2 * r, 0, 2 * r


def copy_all(copies, sems):
    started = []
    for n, (source, target) in enumerate(copies):
        copy = pltpu.make_async_copy(source, target, sems.at[n])
        copy.start()
        started.append(copy)
    for copy in started:
        copy.wait()


def unpack_kernel(position_ref, lines_ref, up_ref, down_ref, sems):
    arrays = (up_ref, down_ref)
    width = lines_ref.shape[1]
    copies = []
    for line, array, start, column, rows in parts_of_line(position_ref[1], width // 32, width):
        at = pl.ds(pl.multiple_of(start, rows), rows)
        copies.append((lines_ref.at[pl.ds(line, rows)], arrays[array].at[at, pl.ds(column, width)]))
    copy_all(copies, sems)


def unpack(lines, position):
    hbm = pl.BlockSpec(memory_space=pltpu.HBM)
    width = lines.shape[1]
    return pl.pallas_call(
        unpack_kernel,
        out_shape=[
            jax.ShapeDtypeStruct((width, 2 * width), bf16),
            jax.ShapeDtypeStruct((2 * width, width), bf16),
        ],
        in_specs=[pl.BlockSpec(memory_space=pltpu.SMEM), hbm],
        out_specs=[hbm, hbm],
        scratch_shapes=[pltpu.SemaphoreType.DMA((96,))],
    )(position, lines)


def pack_kernel(up_ref, down_ref, lines_ref, sems):
    arrays = (up_ref, down_ref)
    width = lines_ref.shape[1]
    copies = []
    for line, array, start, column, rows in parts_of_line(0, width // 32, width):
        source = arrays[array].at[pl.ds(start, rows), pl.ds(column, width)]
        copies.append((source, lines_ref.at[pl.ds(line, rows)]))
    copy_all(copies, sems)


def pack(up, down):
    hbm = pl.BlockSpec(memory_space=pltpu.HBM)
    return pl.pallas_call(
        pack_kernel,
        out_shape=jax.ShapeDtypeStruct((4 * up.shape[0], up.shape[0]), bf16),
        in_specs=[hbm, hbm],
        out_specs=hbm,
        scratch_shapes=[pltpu.SemaphoreType.DMA((96,))],
    )(up, down)


def gather_second(up, down, position):
    width = down.shape[1]
    block = jnp.concatenate([up[:, :width], up[:, width:], down], axis=0)
    other = swap(block, "zh", 1)
    (line,) = stack((block, other))
    return unpack(lax.all_gather(line, ("y", "x"), axis=0, tiled=True), position)


def reduce_second(up, down, zh):
    line = lax.psum_scatter(pack(up, down), ("y", "x"), scatter_dimension=0, tiled=True)
    halves = line.reshape(2, -1, line.shape[1])
    own = add(take(halves, zh), swap(take(halves, 1 - zh), "zh", 1))
    r = own.shape[0] // 4
    return jnp.concatenate([own[:r], own[r : 2 * r]], axis=1), own[2 * r :]


def take(blocks, index):
    return lax.dynamic_index_in_dim(blocks, index, 0, keepdims=False)


def reduce_ring(blocks, axis, at):
    here, ahead, far, behind = (take(blocks, (at + d) % 4) for d in range(4))
    passed = shift(far, axis, 1)
    behind = shift(behind, axis, 3)
    ahead = shift(add(ahead, passed).astype(bf16), axis, 1)
    return add(here, behind, ahead).astype(bf16)


def reduce_direct(blocks, axis, at):
    own = [take(blocks, (at + d) % 4) for d in range(4)]
    moved = [shift(own[d], axis, d) for d in (1, 2, 3)]
    return add(own[0], *moved).astype(bf16)


def reduce_first(up, down, position):
    y, zh, x = position
    r, c = up.shape[0] // 32, up.shape[1]
    b = reduce_ring(jnp.transpose(down.reshape(4, 2, 4, r, c), (2, 1, 0, 3, 4)), "x", x)
    a = reduce_ring(up.reshape(4, 2, 4, r, c), "y", y)
    b = reduce_direct(jnp.transpose(b, (1, 0, 2, 3)), "y", y)
    a = reduce_direct(jnp.transpose(a, (1, 0, 2, 3)), "x", x)
    both = jnp.concatenate([a, b], axis=1)
    own = add(take(both, zh), swap(take(both, 1 - zh), "zh", 1))
    return own[:r], own[r:]


def slot_order(route_ids, experts):
    expert_ids = route_ids[:, 0]
    n = expert_ids.shape[0]
    onehot = (expert_ids[:, None] == jnp.arange(experts, dtype=jnp.int32)[None, :]).astype(bf16)
    row = lax.broadcasted_iota(jnp.int32, (n, n), 0)
    column = lax.broadcasted_iota(jnp.int32, (n, n), 1)
    earlier = jnp.dot((column < row).astype(bf16), onehot, preferred_element_type=f32)
    count = jnp.sum(earlier * onehot.astype(f32), axis=1)
    return expert_ids, count.astype(jnp.int32)


def to_slots(rows, places, slots):
    table = (places[None, :] == jnp.arange(slots, dtype=jnp.int32)[:, None]).astype(rows.dtype)
    return jnp.dot(table, rows, preferred_element_type=f32).astype(rows.dtype)


def from_slots(slot_rows, places):
    slots = slot_rows.shape[0]
    table = (places[:, None] == jnp.arange(slots, dtype=jnp.int32)[None, :]).astype(bf16)
    return jnp.dot(table, slot_rows, preferred_element_type=f32)


def spread_first(slots):
    n = slots.shape[0] // 2
    mine = jnp.concatenate([slots[:n], swap(slots[n:], "zl", 2)], axis=0)
    mine = jnp.concatenate([mine, swap(mine, "zl", 1)], axis=0)
    return jnp.concatenate([mine, swap(mine, "core", 1)], axis=0)


def collect_first(parts):
    for axis in ("core", "zl"):
        n = parts.shape[0] // 2
        parts = add(parts[:n], swap(parts[n:], axis, 1)).astype(bf16)
    n = parts.shape[0] // 2
    return jnp.concatenate([parts[:n], swap(parts[n:], "zl", 2)], axis=0)


def exchange_second(slots):
    blocks = slots.reshape(4, -1, slots.shape[1])
    return lax.all_to_all(blocks, "zl", 0, 0, tiled=True).reshape(slots.shape)


def spread_second(slots):
    mine = exchange_second(slots)
    return jnp.concatenate([mine, swap(mine, "core", 1)], axis=0)


def collect_second(parts):
    n = parts.shape[0] // 2
    own = add(parts[:n], swap(parts[n:], "core", 1)).astype(bf16)
    return exchange_second(own)


def rms_normal(widened):
    return widened * lax.rsqrt(jnp.mean(widened * widened, axis=-1, keepdims=True) + epsilon)


def gelu_slope(pre_gelu):
    _, pullback = jax.vjp(jax.nn.gelu, pre_gelu)
    return pullback(jnp.ones_like(pre_gelu))[0]


def mm(a, b, contract):
    return lax.dot_general(a, b, (contract, ((), ())), preferred_element_type=f32)


def local(tokens, route_first, route_second, up_1, down_1, up_2, down_2, cotangent):
    y, zh, x = (lax.axis_index(a) for a in ("y", "zh", "x"))
    zl = lax.axis_index("zl")
    position = jnp.stack([y, zh, x]).astype(jnp.int32)
    up_1, down_1, up_2, down_2 = up_1[0], down_1[0], up_2[0], down_2[0]

    up_1_full, down_1_full = gather_first(up_1, down_1, position)
    up_2_full, down_2_full = gather_second(up_2, down_2, position)

    n_1, n_2 = 72, 40
    expert_1, count_1 = slot_order(route_first, 2)
    expert_2, count_2 = slot_order(route_second, 4)
    places_1 = (expert_1 ^ (zl // 2)) * n_1 + count_1
    places_2 = expert_2 * n_2 + count_2

    wide_1 = tokens.astype(f32)
    received_1 = spread_first(to_slots(rms_normal(wide_1).astype(bf16), places_1, 2 * n_1))
    arriving_2 = spread_second(to_slots(cotangent, places_2, 4 * n_2))
    pre_1 = mm(received_1, up_1_full, ((1,), (0,)))
    hidden_1 = jax.nn.gelu(pre_1).astype(bf16)
    part_1 = mm(hidden_1, down_1_full, ((1,), (0,))).astype(bf16)
    middle = (wide_1 + from_slots(collect_first(part_1), places_1)).astype(bf16)

    wide_2 = middle.astype(f32)
    received_2 = spread_second(to_slots(rms_normal(wide_2).astype(bf16), places_2, 4 * n_2))
    pre_2 = mm(received_2, up_2_full, ((1,), (0,)))
    hidden_2 = jax.nn.gelu(pre_2).astype(bf16)
    part_2 = mm(hidden_2, down_2_full, ((1,), (0,))).astype(bf16)
    layer_out = (wide_2 + from_slots(collect_second(part_2), places_2)).astype(bf16)

    grad_pre_2 = (mm(arriving_2, down_2_full, ((1,), (1,))) * gelu_slope(pre_2)).astype(bf16)
    grad_slots_2 = mm(grad_pre_2, up_2_full, ((1,), (1,))).astype(bf16)
    grad_down_2 = mm(hidden_2, arriving_2, ((0,), (0,))).astype(bf16)
    grad_up_2 = mm(received_2, grad_pre_2, ((0,), (0,))).astype(bf16)
    grad_normed_2 = from_slots(collect_second(grad_slots_2), places_2)
    _, pullback_2 = jax.vjp(rms_normal, wide_2)
    grad_middle = (cotangent.astype(f32) + pullback_2(grad_normed_2)[0]).astype(bf16)

    arriving_1 = spread_first(to_slots(grad_middle, places_1, 2 * n_1))
    grad_pre_1 = (mm(arriving_1, down_1_full, ((1,), (1,))) * gelu_slope(pre_1)).astype(bf16)
    grad_slots_1 = mm(grad_pre_1, up_1_full, ((1,), (1,))).astype(bf16)
    grad_down_1 = mm(hidden_1, arriving_1, ((0,), (0,))).astype(bf16)
    grad_up_1 = mm(received_1, grad_pre_1, ((0,), (0,))).astype(bf16)
    grad_normed_1 = from_slots(collect_first(grad_slots_1), places_1)
    _, pullback_1 = jax.vjp(rms_normal, wide_1)
    grad_tokens = (grad_middle.astype(f32) + pullback_1(grad_normed_1)[0]).astype(bf16)

    out_up_2, out_down_2 = reduce_second(grad_up_2, grad_down_2, zh)
    out_up_1, out_down_1 = reduce_first(grad_up_1, grad_down_1, (y, zh, x))
    return (layer_out, grad_tokens, out_up_1[None], out_down_1[None], out_up_2[None], out_down_2[None])


def solution(mesh):
    fine = Mesh(mesh.devices.reshape(tuple(SIZES.values())), AXES)
    rows = P(AXES, None)
    weights = P(("zl", "core"), ("y", "zh", "x"), None)
    in_specs = (rows, rows, rows, weights, weights, weights, weights, rows)
    out_specs = (rows, rows, weights, weights, weights, weights)

    return jax.shard_map(local, mesh=fine, in_specs=in_specs, out_specs=out_specs, check_vma=False)
```

```python
import functools

import jax
import jax.numpy as jnp
from jax import lax
from jax.experimental import pallas as pl
from jax.experimental.pallas import tpu as pltpu
from jax.sharding import Mesh, PartitionSpec as P


epsilon = 1e-06
AXES = ("y", "zh", "x", "zl", "core")
SIZES = {"y": 4, "zh": 2, "x": 4, "zl": 4, "core": 2}
bf16, f32 = jnp.bfloat16, jnp.float32


def shift(value, axis, by):
    n = SIZES[axis]
    return lax.ppermute(value, axis, [(i, (i + by) % n) for i in range(n)])


def swap(value, axis, mask):
    return lax.ppermute(value, axis, [(i, i ^ mask) for i in range(SIZES[axis])])


def add(*values):
    total = values[0].astype(f32)
    for v in values[1:]:
        total = total + v.astype(f32)
    return total


def stack_kernel(groups, *refs):
    ins, outs = refs[: sum(groups)], refs[sum(groups) :]
    n = 0
    for count, out in zip(groups, outs):
        rows = out.shape[0] // count
        for k in range(count):
            out[k * rows : (k + 1) * rows, :] = ins[n][...]
            n += 1


def stack(*groups, space=pltpu.VMEM):
    blocks = [block for group in groups for block in group]
    out_shape = [space((len(g) * g[0].shape[0], g[0].shape[1]), g[0].dtype) for g in groups]
    return pl.pallas_call(
        functools.partial(stack_kernel, [len(g) for g in groups]),
        out_shape=out_shape,
        in_specs=[pl.BlockSpec(memory_space=pltpu.VMEM)] * len(blocks),
        out_specs=[pl.BlockSpec(memory_space=pltpu.VMEM)] * len(groups),
        compiler_params=pltpu.CompilerParams(vmem_limit_bytes=8 << 20),
    )(*blocks)


def sources(rows, inner_is_x, position):
    y, zh, x = position
    inner, outer = (x, y) if inner_is_x else (y, x)
    for piece, by in ((0, 0), (1, 3), (2, 1), (3, 2)):
        o = (outer + by) % 4
        for j in range(4):
            i = (inner + 4 - j) % 4
            yy, xx = (o, i) if inner_is_x else (i, o)
            for k in range(2):
                block = yy * 8 + ((zh + k) % 2) * 4 + xx
                yield piece, (j * 2 + k) * rows, block * rows


def assemble_kernel(rows, position_ref, *refs):
    position = (position_ref[0], position_ref[1], position_ref[2])
    for pieces, out_ref, inner_is_x in ((refs[:4], refs[8], True), (refs[4:8], refs[9], False)):
        for which, start, to in sources(rows, inner_is_x, position):
            at = pl.ds(pl.multiple_of(to, rows), rows)
            out_ref[at, :] = pieces[which][start : start + rows, :]


def assemble(first, second, rows, position):
    shape = pltpu.VMEM((32 * rows, first[0].shape[1]), bf16)
    return pl.pallas_call(
        functools.partial(assemble_kernel, rows),
        out_shape=[shape, shape],
        in_specs=[pl.BlockSpec(memory_space=pltpu.SMEM)]
        + [pl.BlockSpec(memory_space=pltpu.VMEM)] * 8,
        out_specs=[pl.BlockSpec(memory_space=pltpu.VMEM)] * 2,
        compiler_params=pltpu.CompilerParams(vmem_limit_bytes=16 << 20),
    )(position, *first, *second)


def gather_first(up, down, position):
    rows = up.shape[0]
    block = jnp.concatenate([up, down], axis=0)
    other = swap(block, "zh", 1)
    a, b = stack((up, other[:rows]), (down, other[rows:]))
    a = [a] + [shift(a, "x", d) for d in (1, 2, 3)]
    b = [b] + [shift(b, "y", d) for d in (1, 2, 3)]
    a, b = stack(a, b)
    a = [a, shift(a, "y", 1), shift(a, "y", 3)]
    b = [b, shift(b, "x", 1), shift(b, "x", 3)]
    a.append(shift(a[1], "y", 1))
    b.append(shift(b[1], "x", 1))
    return assemble(a, b, rows, position)


def parts_of_line(zh, r, width):
    for device in range(16):
        yy, xx = device // 4, device % 4
        for k in range(2):
            block = yy * 8 + ((zh + k) % 2) * 4 + xx
            line = (device * 2 + k) * 4 * r
            yield line, 0, block * r, 0, r
            yield line + r, 0, block * r, width, r
            yield line + 2 * r, 1, block * 2 * r, 0, 2 * r


def copy_all(copies, sems):
    started = []
    for n, (source, target) in enumerate(copies):
        copy = pltpu.make_async_copy(source, target, sems.at[n])
        copy.start()
        started.append(copy)
    for copy in started:
        copy.wait()


def unpack_kernel(position_ref, lines_ref, up_ref, down_ref, sems):
    arrays = (up_ref, down_ref)
    width = lines_ref.shape[1]
    copies = []
    for line, array, start, column, rows in parts_of_line(position_ref[1], width // 32, width):
        at = pl.ds(pl.multiple_of(start, rows), rows)
        copies.append((lines_ref.at[pl.ds(line, rows)], arrays[array].at[at, pl.ds(column, width)]))
    copy_all(copies, sems)


def unpack(lines, position):
    width = lines.shape[1]
    return pl.pallas_call(
        unpack_kernel,
        out_shape=[
            pltpu.VMEM((width, 2 * width), bf16),
            pltpu.VMEM((2 * width, width), bf16),
        ],
        in_specs=[
            pl.BlockSpec(memory_space=pltpu.SMEM),
            pl.BlockSpec(memory_space=pltpu.HBM),
        ],
        out_specs=[pl.BlockSpec(memory_space=pltpu.VMEM)] * 2,
        scratch_shapes=[pltpu.SemaphoreType.DMA((96,))],
        compiler_params=pltpu.CompilerParams(vmem_limit_bytes=16 << 20),
    )(position, lines)


def gather_second(up, down, position):
    width = down.shape[1]
    block = jnp.concatenate([up[:, :width], up[:, width:], down], axis=0)
    other = swap(block, "zh", 1)
    (line,) = stack((block, other), space=jax.ShapeDtypeStruct)
    return unpack(lax.all_gather(line, ("y", "x"), axis=0, tiled=True), position)


def take(blocks, index):
    return lax.dynamic_index_in_dim(blocks, index, 0, keepdims=False)


def reduce_ring(blocks, axis, at, by):
    here, ahead, far, behind = (take(blocks, (at + d * by) % 4) for d in range(4))
    passed = shift(far, axis, by)
    behind = shift(behind, axis, 4 - by)
    ahead = shift(add(ahead, passed).astype(bf16), axis, by)
    return add(here, behind, ahead).astype(bf16)


def reduce_direct(blocks, axis, at):
    own = [take(blocks, (at + d) % 4) for d in range(4)]
    moved = [shift(own[d], axis, d) for d in (1, 2, 3)]
    return add(own[0], *moved).astype(bf16)


def reduce_pair(up, down, position, by):
    y, zh, x = position

    def blocks(value):
        return value.reshape(4, 2, 4, value.shape[0] // 32, value.shape[1])

    b = jnp.transpose(blocks(down), (2, 1, 0, 3, 4))
    b = reduce_ring(b, "x", x, by)
    a = reduce_ring(blocks(up), "y", y, by)
    b = reduce_direct(jnp.transpose(b, (1, 0, 2, 3)), "y", y)
    a = reduce_direct(jnp.transpose(a, (1, 0, 2, 3)), "x", x)
    r, width = a.shape[1], down.shape[1]
    columns = [a[:, :, k : k + width] for k in range(0, a.shape[2], width)]
    both = jnp.concatenate(columns + [b], axis=1)
    own = add(take(both, zh), swap(take(both, 1 - zh), "zh", 1))
    pieces = [own[k * r : (k + 1) * r] for k in range(len(columns))]
    return jnp.concatenate(pieces, axis=1), own[len(columns) * r :]


def slot_order(route_ids, experts):
    expert_ids = route_ids[:, 0]
    n = expert_ids.shape[0]
    onehot = (expert_ids[:, None] == jnp.arange(experts, dtype=jnp.int32)[None, :]).astype(bf16)
    row = lax.broadcasted_iota(jnp.int32, (n, n), 0)
    column = lax.broadcasted_iota(jnp.int32, (n, n), 1)
    earlier = jnp.dot((column < row).astype(bf16), onehot, preferred_element_type=f32)
    count = jnp.sum(earlier * onehot.astype(f32), axis=1)
    return expert_ids, count.astype(jnp.int32)


def to_slots(rows, places, slots):
    table = (places[None, :] == jnp.arange(slots, dtype=jnp.int32)[:, None]).astype(rows.dtype)
    return jnp.dot(table, rows, preferred_element_type=f32).astype(rows.dtype)


def from_slots(slot_rows, places):
    slots = slot_rows.shape[0]
    table = (places[:, None] == jnp.arange(slots, dtype=jnp.int32)[None, :]).astype(bf16)
    return jnp.dot(table, slot_rows, preferred_element_type=f32)


def spread_first(slots):
    n = slots.shape[0] // 2
    mine = jnp.concatenate([slots[:n], swap(slots[n:], "zl", 2)], axis=0)
    mine = jnp.concatenate([mine, swap(mine, "zl", 1)], axis=0)
    return jnp.concatenate([mine, swap(mine, "core", 1)], axis=0)


def collect_first(parts):
    for axis in ("core", "zl"):
        n = parts.shape[0] // 2
        parts = add(parts[:n], swap(parts[n:], axis, 1)).astype(bf16)
    n = parts.shape[0] // 2
    return jnp.concatenate([parts[:n], swap(parts[n:], "zl", 2)], axis=0)


def exchange_second(slots):
    n = slots.shape[0] // 4
    moved = [swap(slots[k * n : (k + 1) * n], "zl", k) for k in (1, 2, 3)]
    return jnp.concatenate([slots[:n]] + moved, axis=0)


def spread_second(slots):
    mine = exchange_second(slots)
    return jnp.concatenate([mine, swap(mine, "core", 1)], axis=0)


def collect_second(parts):
    n = parts.shape[0] // 2
    own = add(parts[:n], swap(parts[n:], "core", 1)).astype(bf16)
    return exchange_second(own)


def rms_normal(widened):
    return widened * lax.rsqrt(jnp.mean(widened * widened, axis=-1, keepdims=True) + epsilon)


def gelu_slope(pre_gelu):
    _, pullback = jax.vjp(jax.nn.gelu, pre_gelu)
    return pullback(jnp.ones_like(pre_gelu))[0]


def mm(a, b, contract):
    return lax.dot_general(a, b, (contract, ((), ())), preferred_element_type=f32)


def local(tokens, route_first, route_second, up_1, down_1, up_2, down_2, cotangent):
    y, zh, x = (lax.axis_index(a) for a in ("y", "zh", "x"))
    zl = lax.axis_index("zl")
    position = jnp.stack([y, zh, x]).astype(jnp.int32)
    up_1, down_1, up_2, down_2 = up_1[0], down_1[0], up_2[0], down_2[0]

    up_1_full, down_1_full = gather_first(up_1, down_1, position)
    up_2_full, down_2_full = gather_second(up_2, down_2, position)

    n_1, n_2 = 72, 40
    expert_1, count_1 = slot_order(route_first, 2)
    expert_2, count_2 = slot_order(route_second, 4)
    places_1 = (expert_1 ^ (zl // 2)) * n_1 + count_1
    places_2 = (expert_2 ^ zl) * n_2 + count_2

    wide_1 = tokens.astype(f32)
    received_1 = spread_first(to_slots(rms_normal(wide_1).astype(bf16), places_1, 2 * n_1))
    arriving_2 = spread_second(to_slots(cotangent, places_2, 4 * n_2))
    pre_1 = mm(received_1, up_1_full, ((1,), (0,)))
    hidden_1 = jax.nn.gelu(pre_1).astype(bf16)
    part_1 = mm(hidden_1, down_1_full, ((1,), (0,))).astype(bf16)
    middle = (wide_1 + from_slots(collect_first(part_1), places_1)).astype(bf16)

    wide_2 = middle.astype(f32)
    received_2 = spread_second(to_slots(rms_normal(wide_2).astype(bf16), places_2, 4 * n_2))
    pre_2 = mm(received_2, up_2_full, ((1,), (0,)))
    hidden_2 = jax.nn.gelu(pre_2).astype(bf16)
    part_2 = mm(hidden_2, down_2_full, ((1,), (0,))).astype(bf16)
    layer_out = (wide_2 + from_slots(collect_second(part_2), places_2)).astype(bf16)

    grad_pre_2 = (mm(arriving_2, down_2_full, ((1,), (1,))) * gelu_slope(pre_2)).astype(bf16)
    grad_slots_2 = mm(grad_pre_2, up_2_full, ((1,), (1,))).astype(bf16)
    grad_down_2 = mm(hidden_2, arriving_2, ((0,), (0,))).astype(bf16)
    grad_up_2 = mm(received_2, grad_pre_2, ((0,), (0,))).astype(bf16)
    grad_normed_2 = from_slots(collect_second(grad_slots_2), places_2)
    _, pullback_2 = jax.vjp(rms_normal, wide_2)
    grad_middle = (cotangent.astype(f32) + pullback_2(grad_normed_2)[0]).astype(bf16)

    arriving_1 = spread_first(to_slots(grad_middle, places_1, 2 * n_1))
    grad_pre_1 = (mm(arriving_1, down_1_full, ((1,), (1,))) * gelu_slope(pre_1)).astype(bf16)
    grad_slots_1 = mm(grad_pre_1, up_1_full, ((1,), (1,))).astype(bf16)
    grad_down_1 = mm(hidden_1, arriving_1, ((0,), (0,))).astype(bf16)
    grad_up_1 = mm(received_1, grad_pre_1, ((0,), (0,))).astype(bf16)
    grad_normed_1 = from_slots(collect_first(grad_slots_1), places_1)
    _, pullback_1 = jax.vjp(rms_normal, wide_1)
    grad_tokens = (grad_middle.astype(f32) + pullback_1(grad_normed_1)[0]).astype(bf16)

    out_up_2, out_down_2 = reduce_pair(grad_up_2, grad_down_2, (y, zh, x), 3)
    out_up_1, out_down_1 = reduce_pair(grad_up_1, grad_down_1, (y, zh, x), 1)
    return (layer_out, grad_tokens, out_up_1[None], out_down_1[None], out_up_2[None], out_down_2[None])


def solution(mesh):
    fine = Mesh(mesh.devices.reshape(tuple(SIZES.values())), AXES)
    rows = P(AXES, None)
    weights = P(("zl", "core"), ("y", "zh", "x"), None)
    in_specs = (rows, rows, rows, weights, weights, weights, weights, rows)
    out_specs = (rows, rows, weights, weights, weights, weights)

    return jax.shard_map(local, mesh=fine, in_specs=in_specs, out_specs=out_specs, check_vma=False)
```

```python
import functools

import jax
import jax.numpy as jnp
from jax import lax
from jax.experimental import pallas as pl
from jax.experimental.pallas import tpu as pltpu
from jax.sharding import Mesh, PartitionSpec as P


epsilon = 1e-06
AXES = ("y", "zh", "x", "zl", "core")
SIZES = {"y": 4, "zh": 2, "x": 4, "zl": 4, "core": 2}
bf16, f32 = jnp.bfloat16, jnp.float32


def shift(value, axis, by):
    n = SIZES[axis]
    return lax.ppermute(value, axis, [(i, (i + by) % n) for i in range(n)])


def swap(value, axis, mask):
    return lax.ppermute(value, axis, [(i, i ^ mask) for i in range(SIZES[axis])])


def add(*values):
    total = values[0].astype(f32)
    for v in values[1:]:
        total = total + v.astype(f32)
    return total


def stack_kernel(groups, *refs):
    ins, outs = refs[: sum(groups)], refs[sum(groups) :]
    n = 0
    for count, out in zip(groups, outs):
        rows = out.shape[0] // count
        for k in range(count):
            out[k * rows : (k + 1) * rows, :] = ins[n][...]
            n += 1


def stack(*groups, space=pltpu.VMEM):
    blocks = [block for group in groups for block in group]
    out_shape = [space((len(g) * g[0].shape[0], g[0].shape[1]), g[0].dtype) for g in groups]
    return pl.pallas_call(
        functools.partial(stack_kernel, [len(g) for g in groups]),
        out_shape=out_shape,
        in_specs=[pl.BlockSpec(memory_space=pltpu.VMEM)] * len(blocks),
        out_specs=[pl.BlockSpec(memory_space=pltpu.VMEM)] * len(groups),
        compiler_params=pltpu.CompilerParams(vmem_limit_bytes=3 << 20),
    )(*blocks)


def sources(rows, inner_is_x, position):
    y, zh, x = position
    inner, outer = (x, y) if inner_is_x else (y, x)
    for piece, by in ((0, 0), (1, 3), (2, 1), (3, 2)):
        o = (outer + by) % 4
        for j in range(4):
            i = (inner + 4 - j) % 4
            yy, xx = (o, i) if inner_is_x else (i, o)
            for k in range(2):
                block = yy * 8 + ((zh + k) % 2) * 4 + xx
                yield piece, (j * 2 + k) * rows, block * rows


def assemble_kernel(rows, position_ref, *refs):
    position = (position_ref[0], position_ref[1], position_ref[2])
    for pieces, out_ref, inner_is_x in ((refs[:4], refs[8], True), (refs[4:8], refs[9], False)):
        for which, start, to in sources(rows, inner_is_x, position):
            at = pl.ds(pl.multiple_of(to, rows), rows)
            out_ref[at, :] = pieces[which][start : start + rows, :]


def assemble(first, second, rows, position):
    shape = pltpu.VMEM((32 * rows, first[0].shape[1]), bf16)
    return pl.pallas_call(
        functools.partial(assemble_kernel, rows),
        out_shape=[shape, shape],
        in_specs=[pl.BlockSpec(memory_space=pltpu.SMEM)]
        + [pl.BlockSpec(memory_space=pltpu.VMEM)] * 8,
        out_specs=[pl.BlockSpec(memory_space=pltpu.VMEM)] * 2,
        compiler_params=pltpu.CompilerParams(vmem_limit_bytes=6 << 20),
    )(position, *first, *second)


def gather_first(up, down, position):
    rows = up.shape[0]
    block = jnp.concatenate([up, down], axis=0)
    other = swap(block, "zh", 1)
    a, b = stack((up, other[:rows]), (down, other[rows:]))
    a = [a] + [shift(a, "x", d) for d in (1, 2, 3)]
    b = [b] + [shift(b, "y", d) for d in (1, 2, 3)]
    a, b = stack(a, b)
    a = [a, shift(a, "y", 1), shift(a, "y", 3)]
    b = [b, shift(b, "x", 1), shift(b, "x", 3)]
    a.append(shift(a[1], "y", 1))
    b.append(shift(b[1], "x", 1))
    return assemble(a, b, rows, position)


def copy_all(copies, sems):
    started = []
    for n, (source, target) in enumerate(copies):
        copy = pltpu.make_async_copy(source, target, sems.at[n])
        copy.start()
        started.append(copy)
    for copy in started:
        copy.wait()


def unpack_kernel(position_ref, lines_ref, up_ref, down_ref, sems):
    r, width = up_ref.shape[2], lines_ref.shape[4]
    copies = []
    for y in range(4):
        for k in range(2):
            to = y * 2 + lax.rem(position_ref[1] + k, 2)
            line = lines_ref.at[y, :, k]
            for column in range(2):
                target = up_ref.at[to, :, :, pl.ds(column * width, width)]
                copies.append((line.at[:, pl.ds(column * r, r)], target))
            copies.append((line.at[:, pl.ds(2 * r, 2 * r)], down_ref.at[to]))
    copy_all(copies, sems)


def unpack(lines, position):
    width = lines.shape[1]
    r = width // 32
    up, down = pl.pallas_call(
        unpack_kernel,
        out_shape=[
            pltpu.VMEM((8, 4, r, 2 * width), bf16),
            pltpu.VMEM((8, 4, 2 * r, width), bf16),
        ],
        in_specs=[
            pl.BlockSpec(memory_space=pltpu.SMEM),
            pl.BlockSpec(memory_space=pltpu.HBM),
        ],
        out_specs=[pl.BlockSpec(memory_space=pltpu.VMEM)] * 2,
        scratch_shapes=[pltpu.SemaphoreType.DMA((24,))],
        compiler_params=pltpu.CompilerParams(vmem_limit_bytes=2 << 20),
    )(position, lines.reshape(4, 4, 2, 4 * r, width))
    return up.reshape(width, 2 * width), down.reshape(2 * width, width)


def gather_second(up, down, position):
    width = down.shape[1]
    block = jnp.concatenate([up[:, :width], up[:, width:], down], axis=0)
    other = swap(block, "zh", 1)
    (line,) = stack((block, other), space=jax.ShapeDtypeStruct)
    return unpack(lax.all_gather(line, ("y", "x"), axis=0, tiled=True), position)


def take(blocks, index):
    return lax.dynamic_index_in_dim(blocks, index, 0, keepdims=False)


def reduce_ring(blocks, axis, at, by):
    here, ahead, far, behind = (take(blocks, (at + d * by) % 4) for d in range(4))
    passed = shift(far, axis, by)
    behind = shift(behind, axis, 4 - by)
    ahead = shift(add(ahead, passed).astype(bf16), axis, by)
    return add(here, behind, ahead).astype(bf16)


def reduce_direct(blocks, axis, at):
    own = [take(blocks, (at + d) % 4) for d in range(4)]
    moved = [shift(own[d], axis, d) for d in (1, 2, 3)]
    return add(own[0], *moved).astype(bf16)


def reduce_pair(up, down, position, by):
    y, zh, x = position

    def blocks(value):
        return value.reshape(4, 2, 4, value.shape[0] // 32, value.shape[1])

    b = jnp.transpose(blocks(down), (2, 1, 0, 3, 4))
    b = reduce_ring(b, "x", x, by)
    a = reduce_ring(blocks(up), "y", y, by)
    b = reduce_direct(jnp.transpose(b, (1, 0, 2, 3)), "y", y)
    a = reduce_direct(jnp.transpose(a, (1, 0, 2, 3)), "x", x)
    r, width = a.shape[1], down.shape[1]
    columns = [a[:, :, k : k + width] for k in range(0, a.shape[2], width)]
    both = jnp.concatenate(columns + [b], axis=1)
    own = add(take(both, zh), swap(take(both, 1 - zh), "zh", 1))
    pieces = [own[k * r : (k + 1) * r] for k in range(len(columns))]
    return jnp.concatenate(pieces, axis=1), own[len(columns) * r :]


def slot_order(route_ids, experts):
    expert_ids = route_ids[:, 0]
    n = expert_ids.shape[0]
    onehot = (expert_ids[:, None] == jnp.arange(experts, dtype=jnp.int32)[None, :]).astype(bf16)
    row = lax.broadcasted_iota(jnp.int32, (n, n), 0)
    column = lax.broadcasted_iota(jnp.int32, (n, n), 1)
    earlier = jnp.dot((column < row).astype(bf16), onehot, preferred_element_type=f32)
    count = jnp.sum(earlier * onehot.astype(f32), axis=1)
    return expert_ids, count.astype(jnp.int32)


def to_slots(rows, places, slots):
    table = (places[None, :] == jnp.arange(slots, dtype=jnp.int32)[:, None]).astype(rows.dtype)
    return jnp.dot(table, rows, preferred_element_type=f32).astype(rows.dtype)


def from_slots(slot_rows, places):
    slots = slot_rows.shape[0]
    table = (places[:, None] == jnp.arange(slots, dtype=jnp.int32)[None, :]).astype(bf16)
    return jnp.dot(table, slot_rows, preferred_element_type=f32)


def spread_first(slots):
    n = slots.shape[0] // 2
    mine = jnp.concatenate([slots[:n], swap(slots[n:], "zl", 2)], axis=0)
    mine = jnp.concatenate([mine, swap(mine, "zl", 1)], axis=0)
    return jnp.concatenate([mine, swap(mine, "core", 1)], axis=0)


def collect_first(parts):
    for axis in ("core", "zl"):
        n = parts.shape[0] // 2
        parts = add(parts[:n], swap(parts[n:], axis, 1)).astype(bf16)
    n = parts.shape[0] // 2
    return jnp.concatenate([parts[:n], swap(parts[n:], "zl", 2)], axis=0)


def exchange_second(slots):
    n = slots.shape[0] // 4
    moved = [swap(slots[k * n : (k + 1) * n], "zl", k) for k in (1, 2, 3)]
    return jnp.concatenate([slots[:n]] + moved, axis=0)


def spread_second(slots):
    mine = exchange_second(slots)
    return jnp.concatenate([mine, swap(mine, "core", 1)], axis=0)


def collect_second(parts):
    n = parts.shape[0] // 2
    own = add(parts[:n], swap(parts[n:], "core", 1)).astype(bf16)
    return exchange_second(own)


def collect_both(first, second):
    n, m = first.shape[0] // 2, second.shape[0] // 2
    other = swap(jnp.concatenate([first[n:], second[m:]], axis=0), "core", 1)
    first = add(first[:n], other[:n]).astype(bf16)
    second = add(second[:m], other[n:]).astype(bf16)
    n, m = n // 2, m // 4
    kept, *blocks = [second[k * m : (k + 1) * m] for k in range(4)]
    one = swap(jnp.concatenate([first[n:], blocks[0]], axis=0), "zl", 1)
    three = swap(blocks[2], "zl", 3)
    first = add(first[:n], one[:n]).astype(bf16)
    h = n // 2
    two = swap(jnp.concatenate([first[h:], blocks[1]], axis=0), "zl", 2)
    return (
        jnp.concatenate([first[:h], two[:h]], axis=0),
        jnp.concatenate([kept, one[n:], two[h:], three], axis=0),
    )


def rms_normal(widened):
    return widened * lax.rsqrt(jnp.mean(widened * widened, axis=-1, keepdims=True) + epsilon)


def gelu_slope(pre_gelu):
    _, pullback = jax.vjp(jax.nn.gelu, pre_gelu)
    return pullback(jnp.ones_like(pre_gelu))[0]


def mm(a, b, contract):
    return lax.dot_general(a, b, (contract, ((), ())), preferred_element_type=f32)


def local(tokens, route_first, route_second, up_1, down_1, up_2, down_2, cotangent):
    y, zh, x = (lax.axis_index(a) for a in ("y", "zh", "x"))
    zl = lax.axis_index("zl")
    position = jnp.stack([y, zh, x]).astype(jnp.int32)
    up_1, down_1, up_2, down_2 = up_1[0], down_1[0], up_2[0], down_2[0]

    up_1_full, down_1_full = gather_first(up_1, down_1, position)
    up_2_full, down_2_full = gather_second(up_2, down_2, position)

    n_1, n_2 = 72, 40
    expert_1, count_1 = slot_order(route_first, 2)
    expert_2, count_2 = slot_order(route_second, 4)
    places_1 = (expert_1 ^ (zl // 2)) * n_1 + count_1
    places_2 = (expert_2 ^ zl) * n_2 + count_2

    wide_1 = tokens.astype(f32)
    received_1 = spread_first(to_slots(rms_normal(wide_1).astype(bf16), places_1, 2 * n_1))
    arriving_2 = spread_second(to_slots(cotangent, places_2, 4 * n_2))
    pre_1 = mm(received_1, up_1_full, ((1,), (0,)))
    hidden_1 = jax.nn.gelu(pre_1).astype(bf16)
    part_1 = mm(hidden_1, down_1_full, ((1,), (0,))).astype(bf16)
    middle = (wide_1 + from_slots(collect_first(part_1), places_1)).astype(bf16)

    wide_2 = middle.astype(f32)
    received_2 = spread_second(to_slots(rms_normal(wide_2).astype(bf16), places_2, 4 * n_2))
    pre_2 = mm(received_2, up_2_full, ((1,), (0,)))
    hidden_2 = jax.nn.gelu(pre_2).astype(bf16)
    part_2 = mm(hidden_2, down_2_full, ((1,), (0,))).astype(bf16)

    grad_pre_2 = (mm(arriving_2, down_2_full, ((1,), (1,))) * gelu_slope(pre_2)).astype(bf16)
    grad_slots_2 = mm(grad_pre_2, up_2_full, ((1,), (1,))).astype(bf16)
    grad_down_2 = mm(hidden_2, arriving_2, ((0,), (0,))).astype(bf16)
    grad_up_2 = mm(received_2, grad_pre_2, ((0,), (0,))).astype(bf16)
    grad_normed_2 = from_slots(collect_second(grad_slots_2), places_2)
    _, pullback_2 = jax.vjp(rms_normal, wide_2)
    grad_middle = (cotangent.astype(f32) + pullback_2(grad_normed_2)[0]).astype(bf16)

    arriving_1 = spread_first(to_slots(grad_middle, places_1, 2 * n_1))
    grad_pre_1 = (mm(arriving_1, down_1_full, ((1,), (1,))) * gelu_slope(pre_1)).astype(bf16)
    grad_slots_1 = mm(grad_pre_1, up_1_full, ((1,), (1,))).astype(bf16)
    grad_down_1 = mm(hidden_1, arriving_1, ((0,), (0,))).astype(bf16)
    grad_up_1 = mm(received_1, grad_pre_1, ((0,), (0,))).astype(bf16)
    grads_1, parts_2 = collect_both(grad_slots_1, part_2)
    layer_out = (wide_2 + from_slots(parts_2, places_2)).astype(bf16)
    grad_normed_1 = from_slots(grads_1, places_1)
    _, pullback_1 = jax.vjp(rms_normal, wide_1)
    grad_tokens = (grad_middle.astype(f32) + pullback_1(grad_normed_1)[0]).astype(bf16)

    out_up_2, out_down_2 = reduce_pair(grad_up_2, grad_down_2, (y, zh, x), 3)
    out_up_1, out_down_1 = reduce_pair(grad_up_1, grad_down_1, (y, zh, x), 1)
    return (layer_out, grad_tokens, out_up_1[None], out_down_1[None], out_up_2[None], out_down_2[None])


def solution(mesh):
    fine = Mesh(mesh.devices.reshape(tuple(SIZES.values())), AXES)
    rows = P(AXES, None)
    weights = P(("zl", "core"), ("y", "zh", "x"), None)
    in_specs = (rows, rows, rows, weights, weights, weights, weights, rows)
    out_specs = (rows, rows, weights, weights, weights, weights)

    return jax.shard_map(local, mesh=fine, in_specs=in_specs, out_specs=out_specs, check_vma=False)
```
